128 devices in a mesh: ex: 32 (over z, x, y_lo), feat: 4 (over y_hi, core).
Axes of the slice: x: 4, y: 4 (y_hi: 2, y_lo: 2; y = y_hi * 2 + y_lo), z: 4, core: 2. Of those that a mesh axis runs over, the one named last changes fastest.
Arguments:
- train_grads: bfloat16 [12288, 16384], P('ex', 'feat'), may hold values from -6 to 6
- projection: bfloat16 [16384, 4096], P('feat', 'ex'), may hold values from -0.046875 to 0.046875
- test_features: bfloat16 [1024, 4096], P('ex', 'feat'), may hold values from -0.09375 to 0.09375
- example_weights: float32 [12288], P('ex'), may hold values from 0.05 to 1
Outputs:
- scores: float32 [1024, 12288], P('feat', 'ex')
- projected: bfloat16 [12288, 4096], P('ex', 'feat')
The draws below stay inside these ranges and needn't reach their ends.
All inputs are finite; a program needn't handle non-finite values.
Results may differ from the reference program's by a relative error of at most 0.0031.
Values may be sent and summed in bfloat16 or wider, within the bound.
A program may use at most 192 MiB of HBM per device.

```python
import math
import jax
import jax.numpy as jnp
from jax import lax

P_SIZE = 16384
K = 4096
NTR = 12288
NTE = 1024


def levels(own_key, shape, split, least, top_value):
    gain = 1.0
    for dim, blocks in split:
        draws = jax.random.uniform(jax.random.fold_in(jax.random.fold_in(own_key, 6), dim), (blocks,), jnp.float32, least / len(split), top_value / len(split))
        gain = gain * jnp.repeat(jnp.exp(draws), shape[dim] // blocks).reshape((-1,) + (1,) * (len(shape) - 1 - dim))
    return gain


def gaussian(key, extent, deviation, reach, cuts=(), kind=jnp.bfloat16):
    entries = deviation * jax.random.normal(key, extent, jnp.float32)
    if cuts:
        entries = entries * levels(key, extent, cuts, -0.22, 0.18)
    return jnp.clip(entries, -reach, reach).astype(kind)


def setup_inputs(seed: int = 0) -> dict:
    splits = jax.random.split(jax.random.key(seed), 5)
    train_grads = gaussian(splits[0], (NTR, P_SIZE), 1.0, 6.0, ((0, 32), (1, 4)))
    projection = gaussian(splits[1], (P_SIZE, K), P_SIZE ** -0.5, 0.046875, ((0, 4), (1, 32)))
    test_features = gaussian(splits[2], (NTE, K), K ** -0.5, 0.09375, ((0, 32), (1, 4)))
    example_weights = jnp.clip(jnp.exp(math.log(1.0) - 2.9957323 * jax.random.uniform(splits[3], (NTR,), jnp.float32) ** levels(splits[3], (NTR,), ((0, 32),), -0.2, 0.2)), 0.05, 1.0)
    return dict(train_grads=train_grads, projection=projection, test_features=test_features, example_weights=example_weights)


def reference(train_grads, projection, test_features, example_weights):
    projected = jnp.dot(train_grads, projection, preferred_element_type=jnp.float32).astype(jnp.bfloat16)
    inner = lax.dot_general(test_features, projected, (((1,), (1,)), ((), ())), preferred_element_type=jnp.float32)
    return inner * example_weights[None, :], projected
```

```python
import functools

import jax
import jax.numpy as jnp
from jax import lax
from jax.experimental import pallas as pl
from jax.experimental.pallas import tpu as pltpu
from jax.sharding import PartitionSpec as P

MESH = pl.DeviceIdType.MESH
ROWS = 384
DEPTH = 4096
HALF = DEPTH // 2
QUARTER = HALF // 2
LANES = 128
STEP = 512


def project_kernel(
    g_hbm, r_hbm, out_ref, buf, gbuf, cst, xrecv, pst, rcv,
    local_sem, send_sem, piece_sem, g_sem, x_sem, rcv_sem,
):
    ex = lax.axis_index("ex")
    ft = lax.axis_index("feat")
    z, x, yl = ex // 8, (ex // 2) % 4, ex % 2
    yh, c = ft // 2, ft % 2

    def at(dx=0, dz=0, flip_lo=0, flip_hi=0, flip_core=0):
        lo = 1 - yl if flip_lo else yl
        hi = 1 - yh if flip_hi else yh
        core = 1 - c if flip_core else c
        return (((z + dz) % 4) * 8 + ((x + dx) % 4) * 2 + lo, hi * 2 + core)

    first = ("x", "z")
    second = ("z", "x")

    def neighbour(axis, way):
        return at(dx=way) if axis == "x" else at(dz=way)

    pair, twin, opposite, diagonal = (
        at(flip_lo=1), at(flip_core=1), at(flip_hi=1), at(flip_lo=1, flip_hi=1)
    )
    sent = []

    def send(src, dst, sem, device):
        copy = pltpu.make_async_remote_copy(
            src, dst, send_sem.at[len(sent)], sem, device_id=device, device_id_type=MESH
        )
        copy.start()
        sent.append(copy)

    own_r = []
    for h in range(2):
        copy = pltpu.make_async_copy(
            r_hbm.at[pl.ds(h * HALF, HALF)], buf.at[h, 0, 0], local_sem.at[h]
        )
        copy.start()
        own_r.append(copy)
    own_g = pltpu.make_async_copy(g_hbm, gbuf.at[0], local_sem.at[2])
    own_g.start()

    barrier = pltpu.get_barrier_semaphore()
    friends = [at(dx=1), at(dx=-1), at(dz=1), at(dz=-1), pair, twin, opposite, diagonal]
    for device in friends:
        pl.semaphore_signal(barrier, inc=1, device_id=device, device_id_type=MESH)
    pl.semaphore_wait(barrier, len(friends))

    def sem_of(h, a, b):
        return piece_sem.at[h * 16 + a * 4 + b]

    def hop(h, axis, a, b, way, part=None):
        if axis == 0:
            a2, b2 = (a + way) % 4, b
        else:
            a2, b2 = a, (b + way) % 4
        src, dst = buf.at[h, a, b], buf.at[h, a2, b2]
        if part is not None:
            rows = pl.ds(part * QUARTER, QUARTER)
            src, dst = src.at[rows], dst.at[rows]
        send(src, dst, sem_of(h, a2, b2), neighbour((first, second)[axis][h], way))

    def arrived(h, a, b):
        ref = buf.at[h, a, b]
        pltpu.make_async_remote_copy(
            ref, ref, send_sem.at[0], sem_of(h, a, b), device_id=twin, device_id_type=MESH
        ).wait_recv()

    def each(a, b):
        for h in range(2):
            arrived(h, a, b)

    for h in range(2):
        own_r[h].wait()
        for way in (1, -1):
            hop(h, 0, 0, 0, way)
    for h in range(2):
        for way in (1, -1):
            hop(h, 1, 0, 0, way)
    own_g.wait()
    send(gbuf.at[0], gbuf.at[1], g_sem.at[0], pair)

    mine = (c + z) % 2
    keeps_first = ((z - mine + 4) % 4) // 2 == yh
    kept = jnp.where(keeps_first, 0, 1)

    def multiply(s, dx, p):
        item = dx * 2 + p

        def rows_at(i, carry):
            rows = pl.ds(pl.multiple_of(i * LANES, LANES), LANES)
            acc = jnp.zeros((LANES, 2 * LANES), jnp.float32)
            for h in range(2):
                for k in range(0, HALF, STEP):
                    ks = pl.ds(k, STEP)
                    pieces = [
                        buf[0, dx, 2 * p + i, ks, :] if h == 0 else buf[1, 2 * p + i, dx, ks, :]
                        for i in range(2)
                    ]
                    acc += jnp.dot(
                        gbuf[s, rows, pl.ds(h * HALF + k, STEP)],
                        jnp.concatenate(pieces, axis=1),
                        preferred_element_type=jnp.float32,
                    )
            cst[s, item, 0, rows, :] = acc[:, :LANES]
            cst[s, item, 1, rows, :] = acc[:, LANES:]
            return carry

        lax.fori_loop(0, ROWS // LANES, rows_at, 0)
        send(cst.at[s, item, 1 - mine], xrecv.at[s, item], x_sem.at[s * 8 + item], twin)

    given = []

    def add_twin(s, dx, p):
        item = dx * 2 + p
        ref = xrecv.at[s, item]
        pltpu.make_async_remote_copy(
            ref, ref, send_sem.at[0], x_sem.at[s * 8 + item], device_id=twin, device_id_type=MESH
        ).wait_recv()
        total = cst[s, item, mine] + xrecv[s, item]
        pst[s, item] = total.astype(jnp.bfloat16)
        keep = kept == p
        if s == 0:
            cst[s, item, mine] = total
            copy = pltpu.make_async_remote_copy(
                pst.at[s, item], rcv.at[0, dx], send_sem.at[len(sent)], rcv_sem.at[dx],
                device_id=opposite, device_id_type=MESH,
            )
            sent.append(None)

            @pl.when(jnp.logical_not(keep))
            def _():
                copy.start()

            given.append((copy, keep))
        else:
            slot = jnp.where(keep, 1, 2)
            hi = jnp.where(keep, yh, 1 - yh)
            send(
                pst.at[s, item], rcv.at[slot, dx], rcv_sem.at[slot * 4 + dx],
                (pair[0], hi * 2 + c),
            )

    def finish(dx):
        for k in range(3):
            ref = rcv.at[k, dx]
            pltpu.make_async_remote_copy(
                ref, ref, send_sem.at[0], rcv_sem.at[k * 4 + dx], device_id=twin, device_id_type=MESH
            ).wait_recv()
        chunk = ((x - dx + 4) % 4) * 2
        own = cst[0, dx * 2 + kept, mine] + rcv[0, dx].astype(jnp.float32)
        other = rcv[1, dx].astype(jnp.float32) + rcv[2, dx].astype(jnp.float32)
        lanes = pl.ds(pl.multiple_of((chunk + yl) * LANES, LANES), LANES)
        out_ref[:, lanes] = own.astype(jnp.bfloat16)
        lanes = pl.ds(pl.multiple_of((chunk + 1 - yl) * LANES, LANES), LANES)
        out_ref[:, lanes] = other.astype(jnp.bfloat16)

    each(1, 0)
    each(3, 0)
    for h in range(2):
        hop(h, 0, 1, 0, 1, part=0)
        hop(h, 0, 3, 0, -1, part=1)
    for a in (1, 3):
        for h in range(2):
            for way in (1, -1):
                hop(h, 1, a, 0, way)
    each(0, 1)
    each(0, 3)
    for h in range(2):
        hop(h, 1, 0, 1, 1, part=0)
        hop(h, 1, 0, 3, -1, part=1)
    multiply(0, 0, 0)
    each(2, 0)
    for h in range(2):
        for way in (1, -1):
            hop(h, 1, 2, 0, way)
    add_twin(0, 0, 0)
    for a in (1, 3):
        each(a, 1)
        each(a, 3)
        for h in range(2):
            hop(h, 1, a, 1, 1, part=0)
            hop(h, 1, a, 3, -1, part=1)
        if a == 1:
            multiply(0, 1, 0)
    add_twin(0, 1, 0)
    multiply(0, 3, 0)
    each(0, 2)
    multiply(0, 0, 1)
    add_twin(0, 3, 0)
    each(2, 1)
    each(2, 3)
    for h in range(2):
        hop(h, 1, 2, 1, 1, part=0)
        hop(h, 1, 2, 3, -1, part=1)
    add_twin(0, 0, 1)
    each(1, 2)
    multiply(0, 2, 0)
    multiply(0, 1, 1)
    add_twin(0, 2, 0)
    add_twin(0, 1, 1)
    ref = gbuf.at[1]
    pltpu.make_async_remote_copy(
        ref, ref, send_sem.at[0], g_sem.at[0], device_id=twin, device_id_type=MESH
    ).wait_recv()
    before = None
    for now in ((0, 0), (0, 1), (1, 0), (1, 1), (3, 0), (2, 0)):
        multiply(1, *now)
        if before is not None:
            add_twin(1, *before)
        before = now
    each(3, 2)
    multiply(0, 3, 1)
    add_twin(1, *before)
    multiply(1, 3, 1)
    add_twin(0, 3, 1)
    finish(0)
    add_twin(1, 3, 1)
    finish(1)
    each(2, 2)
    multiply(0, 2, 1)
    multiply(1, 2, 1)
    add_twin(0, 2, 1)
    add_twin(1, 2, 1)
    finish(3)
    finish(2)
    for copy in sent:
        if copy is not None:
            copy.wait_send()
    for copy, keep in given:
        @pl.when(jnp.logical_not(keep))
        def _():
            copy.wait_send()


def project(train_grads, projection):
    flops = 2 * 2 * ROWS * DEPTH * 2048
    return pl.pallas_call(
        project_kernel,
        out_shape=jax.ShapeDtypeStruct((ROWS, 1024), jnp.bfloat16),
        in_specs=[pl.BlockSpec(memory_space=pl.ANY)] * 2,
        out_specs=pl.BlockSpec(memory_space=pltpu.VMEM),
        scratch_shapes=[
            pltpu.VMEM((2, 4, 4, HALF, LANES), jnp.bfloat16),
            pltpu.VMEM((2, ROWS, DEPTH), jnp.bfloat16),
            pltpu.VMEM((2, 8, 2, ROWS, LANES), jnp.float32),
            pltpu.VMEM((2, 8, ROWS, LANES), jnp.float32),
            pltpu.VMEM((2, 8, ROWS, LANES), jnp.bfloat16),
            pltpu.VMEM((3, 4, ROWS, LANES), jnp.bfloat16),
            pltpu.SemaphoreType.DMA((3,)),
            pltpu.SemaphoreType.DMA((96,)),
            pltpu.SemaphoreType.DMA((32,)),
            pltpu.SemaphoreType.DMA((1,)),
            pltpu.SemaphoreType.DMA((16,)),
            pltpu.SemaphoreType.DMA((12,)),
        ],
        compiler_params=pltpu.CompilerParams(
            collective_id=0, has_side_effects=True, vmem_limit_bytes=60 * 1024 * 1024
        ),
        cost_estimate=pl.CostEstimate(
            flops=flops * 8, bytes_accessed=8 * 2**20, transcendentals=0
        ),
    )(train_grads, projection)


def local(train_grads, projection, test_features, example_weights):
    projected = project(train_grads, projection)
    tests = lax.all_gather(test_features, "ex", axis=0, tiled=True)
    partial_scores = lax.dot_general(
        tests, projected, (((1,), (1,)), ((), ())), preferred_element_type=jnp.float32
    )
    pieces = lax.all_to_all(partial_scores.reshape(4, 256, ROWS), "feat", 0, 0, tiled=True)
    return jnp.sum(pieces, axis=0) * example_weights[None, :], projected


def solution(mesh):
    return jax.shard_map(
        local,
        mesh=mesh,
        in_specs=(P("ex", "feat"), P("feat", "ex"), P("ex", "feat"), P("ex")),
        out_specs=(P("feat", "ex"), P("ex", "feat")),
        check_vma=False,
    )
```

```python
import jax
import jax.numpy as jnp
from jax import lax
from jax.experimental import pallas as pl
from jax.experimental.pallas import tpu as pltpu
from jax.sharding import PartitionSpec as P

MESH = pl.DeviceIdType.MESH
ROWS = 384
TESTS = 32
DEPTH = 4096
HALF = DEPTH // 2
QUARTER = HALF // 2
LANES = 128
STEP = 512


def project_kernel(
    g_hbm, r_hbm, t_hbm, w_ref, score_ref, out_ref, buf, gbuf, cst, xrecv, pst, rcv,
    tall, part_scores, twin_scores, far_scores,
    local_sem, send_sem, piece_sem, g_sem, x_sem, rcv_sem, t_sem, score_sem,
):
    ex = lax.axis_index("ex")
    ft = lax.axis_index("feat")
    z, x, yl = ex // 8, (ex // 2) % 4, ex % 2
    yh, c = ft // 2, ft % 2

    def at(dx=0, dz=0, flip_lo=0, flip_hi=0, flip_core=0):
        lo = 1 - yl if flip_lo else yl
        hi = 1 - yh if flip_hi else yh
        core = 1 - c if flip_core else c
        return (((z + dz) % 4) * 8 + ((x + dx) % 4) * 2 + lo, hi * 2 + core)

    first = ("x", "z")
    second = ("z", "x")

    def neighbour(axis, way):
        return at(dx=way) if axis == "x" else at(dz=way)

    pair, twin, opposite, diagonal = (
        at(flip_lo=1), at(flip_core=1), at(flip_hi=1), at(flip_lo=1, flip_hi=1)
    )
    sent = []

    def send(src, dst, sem, device):
        copy = pltpu.make_async_remote_copy(
            src, dst, send_sem.at[len(sent)], sem, device_id=device, device_id_type=MESH
        )
        copy.start()
        sent.append(copy)

    own_r = []
    for h in range(2):
        copy = pltpu.make_async_copy(
            r_hbm.at[pl.ds(h * HALF, HALF)], buf.at[h, 0, 0], local_sem.at[h]
        )
        copy.start()
        own_r.append(copy)
    own_g = pltpu.make_async_copy(g_hbm, gbuf.at[0], local_sem.at[2])
    own_g.start()

    def test_rows(h, a, b):
        dx, dz = (a, b) if h == 0 else (b, a)
        lo = yl if h == 0 else 1 - yl
        source = ((z - dz + 4) % 4) * 8 + ((x - dx + 4) % 4) * 2 + lo
        return pl.multiple_of(source * TESTS, TESTS)

    own_t = pltpu.make_async_copy(
        t_hbm, tall.at[pl.ds(test_rows(0, 0, 0), TESTS)], local_sem.at[3]
    )
    own_t.start()

    barrier = pltpu.get_barrier_semaphore()
    friends = [at(dx=1), at(dx=-1), at(dz=1), at(dz=-1), pair, twin, opposite, diagonal]
    for device in friends:
        pl.semaphore_signal(barrier, inc=1, device_id=device, device_id_type=MESH)
    pl.semaphore_wait(barrier, len(friends))

    def sem_of(h, a, b):
        return piece_sem.at[h * 16 + a * 4 + b]

    def hop(h, axis, a, b, way, part=None):
        if axis == 0:
            a2, b2 = (a + way) % 4, b
        else:
            a2, b2 = a, (b + way) % 4
        src, dst = buf.at[h, a, b], buf.at[h, a2, b2]
        if part is not None:
            rows = pl.ds(part * QUARTER, QUARTER)
            src, dst = src.at[rows], dst.at[rows]
        send(src, dst, sem_of(h, a2, b2), neighbour((first, second)[axis][h], way))

    def arrived(h, a, b):
        ref = buf.at[h, a, b]
        pltpu.make_async_remote_copy(
            ref, ref, send_sem.at[0], sem_of(h, a, b), device_id=twin, device_id_type=MESH
        ).wait_recv()

    def test_hop(h, axis, a, b, way, part=None):
        a2, b2 = ((a + way) % 4, b) if axis == 0 else (a, (b + way) % 4)
        start, count = test_rows(h, a, b), TESTS
        if part is not None:
            start, count = pl.multiple_of(start + part * (TESTS // 2), TESTS // 2), TESTS // 2
        rows = pl.ds(start, count)
        send(
            tall.at[rows], tall.at[rows], t_sem.at[h * 16 + a2 * 4 + b2],
            neighbour((first, second)[axis][h], way),
        )

    def tests_arrived(h, a, b):
        ref = tall.at[pl.ds(test_rows(h, a, b), TESTS)]
        pltpu.make_async_remote_copy(
            ref, ref, send_sem.at[0], t_sem.at[h * 16 + a * 4 + b], device_id=twin,
            device_id_type=MESH,
        ).wait_recv()

    def each(a, b):
        for h in range(2):
            arrived(h, a, b)

    for h in range(2):
        own_r[h].wait()
        for way in (1, -1):
            hop(h, 0, 0, 0, way)
    for h in range(2):
        for way in (1, -1):
            hop(h, 1, 0, 0, way)
    own_t.wait()
    rows = pl.ds(test_rows(0, 0, 0), TESTS)
    send(tall.at[rows], tall.at[rows], t_sem.at[16], pair)
    own_g.wait()
    send(gbuf.at[0], gbuf.at[1], g_sem.at[0], pair)

    mine = (c + z) % 2
    keeps_first = ((z - mine + 4) % 4) // 2 == yh
    kept = jnp.where(keeps_first, 0, 1)

    def multiply(s, dx, p):
        item = dx * 2 + p

        def rows_at(i, carry):
            rows = pl.ds(pl.multiple_of(i * LANES, LANES), LANES)
            acc = jnp.zeros((LANES, 2 * LANES), jnp.float32)
            for h in range(2):
                for k in range(0, HALF, STEP):
                    ks = pl.ds(k, STEP)
                    pieces = [
                        buf[0, dx, 2 * p + i, ks, :] if h == 0 else buf[1, 2 * p + i, dx, ks, :]
                        for i in range(2)
                    ]
                    acc += jnp.dot(
                        gbuf[s, rows, pl.ds(h * HALF + k, STEP)],
                        jnp.concatenate(pieces, axis=1),
                        preferred_element_type=jnp.float32,
                    )
            cst[s, item, 0, rows, :] = acc[:, :LANES]
            cst[s, item, 1, rows, :] = acc[:, LANES:]
            return carry

        lax.fori_loop(0, ROWS // LANES, rows_at, 0)
        send(cst.at[s, item, 1 - mine], xrecv.at[s, item], x_sem.at[s * 8 + item], twin)

    given = []

    def add_twin(s, dx, p):
        item = dx * 2 + p
        ref = xrecv.at[s, item]
        pltpu.make_async_remote_copy(
            ref, ref, send_sem.at[0], x_sem.at[s * 8 + item], device_id=twin, device_id_type=MESH
        ).wait_recv()
        total = cst[s, item, mine] + xrecv[s, item]
        pst[s, item] = total.astype(jnp.bfloat16)
        keep = kept == p
        if s == 0:
            cst[s, item, mine] = total
            copy = pltpu.make_async_remote_copy(
                pst.at[s, item], rcv.at[0, dx], send_sem.at[len(sent)], rcv_sem.at[dx],
                device_id=opposite, device_id_type=MESH,
            )
            sent.append(None)

            @pl.when(jnp.logical_not(keep))
            def _():
                copy.start()

            given.append((copy, keep))
        else:
            slot = jnp.where(keep, 1, 2)
            hi = jnp.where(keep, yh, 1 - yh)
            send(
                pst.at[s, item], rcv.at[slot, dx], rcv_sem.at[slot * 4 + dx],
                (pair[0], hi * 2 + c),
            )

    def finish(dx):
        for k in range(3):
            ref = rcv.at[k, dx]
            pltpu.make_async_remote_copy(
                ref, ref, send_sem.at[0], rcv_sem.at[k * 4 + dx], device_id=twin, device_id_type=MESH
            ).wait_recv()
        chunk = ((x - dx + 4) % 4) * 2
        own = cst[0, dx * 2 + kept, mine] + rcv[0, dx].astype(jnp.float32)
        other = rcv[1, dx].astype(jnp.float32) + rcv[2, dx].astype(jnp.float32)
        lanes = pl.ds(pl.multiple_of((chunk + yl) * LANES, LANES), LANES)
        out_ref[:, lanes] = own.astype(jnp.bfloat16)
        lanes = pl.ds(pl.multiple_of((chunk + 1 - yl) * LANES, LANES), LANES)
        out_ref[:, lanes] = other.astype(jnp.bfloat16)

    each(1, 0)
    each(3, 0)
    for h in range(2):
        hop(h, 0, 1, 0, 1, part=0)
        hop(h, 0, 3, 0, -1, part=1)
    for a in (1, 3):
        for h in range(2):
            for way in (1, -1):
                hop(h, 1, a, 0, way)
    each(0, 1)
    each(0, 3)
    for h in range(2):
        hop(h, 1, 0, 1, 1, part=0)
        hop(h, 1, 0, 3, -1, part=1)
    tests_arrived(1, 0, 0)
    for axis in range(2):
        for h in range(2):
            for way in (1, -1):
                test_hop(h, axis, 0, 0, way)
    multiply(0, 0, 0)
    each(2, 0)
    for h in range(2):
        for way in (1, -1):
            hop(h, 1, 2, 0, way)
    add_twin(0, 0, 0)
    for a in (1, 3):
        each(a, 1)
        each(a, 3)
        for h in range(2):
            hop(h, 1, a, 1, 1, part=0)
            hop(h, 1, a, 3, -1, part=1)
        if a == 1:
            multiply(0, 1, 0)
    for a in (1, 3):
        for h in range(2):
            tests_arrived(h, a, 0)
            tests_arrived(h, 0, a)
            way = 1 if a == 1 else -1
            test_hop(h, 0, a, 0, way, part=a // 2)
            test_hop(h, 1, 0, a, way, part=a // 2)
    add_twin(0, 1, 0)
    multiply(0, 3, 0)
    each(0, 2)
    multiply(0, 0, 1)
    add_twin(0, 3, 0)
    each(2, 1)
    each(2, 3)
    for h in range(2):
        hop(h, 1, 2, 1, 1, part=0)
        hop(h, 1, 2, 3, -1, part=1)
    for h in range(2):
        tests_arrived(h, 2, 0)
    for a in (1, 3, 2):
        for h in range(2):
            for way in (1, -1):
                test_hop(h, 1, a, 0, way)
    add_twin(0, 0, 1)
    each(1, 2)
    multiply(0, 2, 0)
    multiply(0, 1, 1)
    add_twin(0, 2, 0)
    add_twin(0, 1, 1)
    ref = gbuf.at[1]
    pltpu.make_async_remote_copy(
        ref, ref, send_sem.at[0], g_sem.at[0], device_id=twin, device_id_type=MESH
    ).wait_recv()
    before = None
    for now in ((0, 0), (0, 1), (1, 0), (1, 1), (3, 0), (2, 0)):
        multiply(1, *now)
        if before is not None:
            add_twin(1, *before)
        before = now
    each(3, 2)
    multiply(0, 3, 1)
    add_twin(1, *before)
    multiply(1, 3, 1)
    add_twin(0, 3, 1)
    finish(0)
    add_twin(1, 3, 1)
    finish(1)
    each(2, 2)
    for a in (1, 3, 2):
        for h in range(2):
            tests_arrived(h, a, 1)
            tests_arrived(h, a, 3)
            test_hop(h, 1, a, 1, 1, part=0)
            test_hop(h, 1, a, 3, -1, part=1)
    multiply(0, 2, 1)
    multiply(1, 2, 1)
    add_twin(0, 2, 1)
    add_twin(1, 2, 1)
    finish(3)
    for h in range(2):
        for a in range(4):
            tests_arrived(h, a, 2)
    finish(2)

    def score(quarter):
        def tile(i, carry):
            rows = pl.ds(pl.multiple_of(quarter * 256 + i * LANES, LANES), LANES)
            part_scores[quarter, pl.ds(pl.multiple_of(i * LANES, LANES), LANES), :] = (
                lax.dot_general(
                    tall[rows, :], out_ref[...], (((1,), (1,)), ((), ())),
                    preferred_element_type=jnp.float32,
                )
            )
            return carry

        lax.fori_loop(0, 2, tile, 0)

    def twin_sum(quarter, k):
        ref = twin_scores.at[k]
        pltpu.make_async_remote_copy(
            ref, ref, send_sem.at[0], score_sem.at[k], device_id=twin, device_id_type=MESH
        ).wait_recv()
        return part_scores[quarter] + twin_scores[k]

    far, near = (1 - yh) * 2, yh * 2
    score(far + 1 - c)
    send(part_scores.at[far + 1 - c], twin_scores.at[0], score_sem.at[0], twin)
    score(far + c)
    part_scores[far + c] = twin_sum(far + c, 0)
    send(part_scores.at[far + c], far_scores, score_sem.at[2], opposite)
    score(near + 1 - c)
    send(part_scores.at[near + 1 - c], twin_scores.at[1], score_sem.at[1], twin)
    score(near + c)
    total = twin_sum(near + c, 1)
    pltpu.make_async_remote_copy(
        far_scores, far_scores, send_sem.at[0], score_sem.at[2], device_id=twin,
        device_id_type=MESH,
    ).wait_recv()
    score_ref[...] = (total + far_scores[...]) * w_ref[...]
    for copy in sent:
        if copy is not None:
            copy.wait_send()
    for copy, keep in given:
        @pl.when(jnp.logical_not(keep))
        def _():
            copy.wait_send()


def local(train_grads, projection, test_features, example_weights):
    flops = 2 * 2 * ROWS * DEPTH * 2048
    return pl.pallas_call(
        project_kernel,
        out_shape=(
            jax.ShapeDtypeStruct((256, ROWS), jnp.float32),
            jax.ShapeDtypeStruct((ROWS, 1024), jnp.bfloat16),
        ),
        in_specs=[pl.BlockSpec(memory_space=pl.ANY)] * 3
        + [pl.BlockSpec(memory_space=pltpu.VMEM)],
        out_specs=(pl.BlockSpec(memory_space=pltpu.VMEM),) * 2,
        scratch_shapes=[
            pltpu.VMEM((2, 4, 4, HALF, LANES), jnp.bfloat16),
            pltpu.VMEM((2, ROWS, DEPTH), jnp.bfloat16),
            pltpu.VMEM((2, 8, 2, ROWS, LANES), jnp.float32),
            pltpu.VMEM((2, 8, ROWS, LANES), jnp.float32),
            pltpu.VMEM((2, 8, ROWS, LANES), jnp.bfloat16),
            pltpu.VMEM((3, 4, ROWS, LANES), jnp.bfloat16),
            pltpu.VMEM((1024, 1024), jnp.bfloat16),
            pltpu.VMEM((4, 256, ROWS), jnp.float32),
            pltpu.VMEM((2, 256, ROWS), jnp.float32),
            pltpu.VMEM((256, ROWS), jnp.float32),
            pltpu.SemaphoreType.DMA((4,)),
            pltpu.SemaphoreType.DMA((136,)),
            pltpu.SemaphoreType.DMA((32,)),
            pltpu.SemaphoreType.DMA((1,)),
            pltpu.SemaphoreType.DMA((16,)),
            pltpu.SemaphoreType.DMA((12,)),
            pltpu.SemaphoreType.DMA((32,)),
            pltpu.SemaphoreType.DMA((3,)),
        ],
        compiler_params=pltpu.CompilerParams(
            collective_id=0, has_side_effects=True, vmem_limit_bytes=60 * 1024 * 1024
        ),
        cost_estimate=pl.CostEstimate(
            flops=flops, bytes_accessed=8 * 2**20, transcendentals=0
        ),
    )(train_grads, projection, test_features, example_weights.reshape(1, ROWS))


def solution(mesh):
    return jax.shard_map(
        local,
        mesh=mesh,
        in_specs=(P("ex", "feat"), P("feat", "ex"), P("ex", "feat"), P("ex")),
        out_specs=(P("feat", "ex"), P("ex", "feat")),
        check_vma=False,
    )
```

```python
import jax
import jax.numpy as jnp
from jax import lax
from jax.experimental import pallas as pl
from jax.experimental.pallas import tpu as pltpu
from jax.sharding import PartitionSpec as P

MESH = pl.DeviceIdType.MESH
ROWS = 384
TESTS = 32
TILE = 192
TILES = ROWS // TILE
DEPTH = 4096
HALF = DEPTH // 2
QUARTER = HALF // 2
LANES = 128
STEP = 512


def project_kernel(
    g_hbm, r_hbm, t_hbm, score_ref, out_ref, buf, gbuf, cst, xrecv, pst, rcv,
    tall, part_scores, twin_scores, relay_scores, far_scores,
    local_sem, send_sem, piece_sem, g_sem, x_sem, rcv_sem, t_sem, score_sem,
):
    ex = lax.axis_index("ex")
    ft = lax.axis_index("feat")
    z, x, yl = ex // 8, (ex // 2) % 4, ex % 2
    yh, c = ft // 2, ft % 2

    def at(dx=0, dz=0, flip_lo=0, flip_hi=0, flip_core=0):
        lo = 1 - yl if flip_lo else yl
        hi = 1 - yh if flip_hi else yh
        core = 1 - c if flip_core else c
        return (((z + dz) % 4) * 8 + ((x + dx) % 4) * 2 + lo, hi * 2 + core)

    first = ("x", "z")
    second = ("z", "x")

    def neighbour(axis, way):
        return at(dx=way) if axis == "x" else at(dz=way)

    pair, twin, opposite, diagonal = (
        at(flip_lo=1), at(flip_core=1), at(flip_hi=1), at(flip_lo=1, flip_hi=1)
    )
    sent = []

    def send(src, dst, sem, device):
        copy = pltpu.make_async_remote_copy(
            src, dst, send_sem.at[len(sent)], sem, device_id=device, device_id_type=MESH
        )
        copy.start()
        sent.append(copy)

    own_r = []
    for h in range(2):
        copy = pltpu.make_async_copy(
            r_hbm.at[pl.ds(h * HALF, HALF)], buf.at[h, 0, 0], local_sem.at[h]
        )
        copy.start()
        own_r.append(copy)
    own_g = pltpu.make_async_copy(g_hbm, gbuf.at[0], local_sem.at[2])
    own_g.start()

    def test_rows(h, a, b):
        dx, dz = (a, b) if h == 0 else (b, a)
        lo = yl if h == 0 else 1 - yl
        source = ((z - dz + 4) % 4) * 8 + ((x - dx + 4) % 4) * 2 + lo
        return pl.multiple_of(source * TESTS, TESTS)

    own_t = pltpu.make_async_copy(
        t_hbm, tall.at[pl.ds(test_rows(0, 0, 0), TESTS)], local_sem.at[3]
    )
    own_t.start()

    barrier = pltpu.get_barrier_semaphore()
    friends = [at(dx=1), at(dx=-1), at(dz=1), at(dz=-1), pair, twin, opposite, diagonal]
    for device in friends:
        pl.semaphore_signal(barrier, inc=1, device_id=device, device_id_type=MESH)
    pl.semaphore_wait(barrier, len(friends))

    def sem_of(h, a, b):
        return piece_sem.at[h * 16 + a * 4 + b]

    def hop(h, axis, a, b, way, part=None):
        if axis == 0:
            a2, b2 = (a + way) % 4, b
        else:
            a2, b2 = a, (b + way) % 4
        src, dst = buf.at[h, a, b], buf.at[h, a2, b2]
        if part is not None:
            rows = pl.ds(part * QUARTER, QUARTER)
            src, dst = src.at[rows], dst.at[rows]
        send(src, dst, sem_of(h, a2, b2), neighbour((first, second)[axis][h], way))

    def arrived(h, a, b):
        ref = buf.at[h, a, b]
        pltpu.make_async_remote_copy(
            ref, ref, send_sem.at[0], sem_of(h, a, b), device_id=twin, device_id_type=MESH
        ).wait_recv()

    def test_hop(h, axis, a, b, way, part=None):
        a2, b2 = ((a + way) % 4, b) if axis == 0 else (a, (b + way) % 4)
        start, count = test_rows(h, a, b), TESTS
        if part is not None:
            start, count = pl.multiple_of(start + part * (TESTS // 2), TESTS // 2), TESTS // 2
        rows = pl.ds(start, count)
        send(
            tall.at[rows], tall.at[rows], t_sem.at[h * 16 + a2 * 4 + b2],
            neighbour((first, second)[axis][h], way),
        )

    def tests_arrived(h, a, b):
        ref = tall.at[pl.ds(test_rows(h, a, b), TESTS)]
        pltpu.make_async_remote_copy(
            ref, ref, send_sem.at[0], t_sem.at[h * 16 + a * 4 + b], device_id=twin,
            device_id_type=MESH,
        ).wait_recv()

    def landed(ref, sem):
        pltpu.make_async_remote_copy(
            ref, ref, send_sem.at[0], sem, device_id=twin, device_id_type=MESH
        ).wait_recv()

    def each(a, b):
        for h in range(2):
            arrived(h, a, b)

    for h in range(2):
        own_r[h].wait()
        for way in (1, -1):
            hop(h, 0, 0, 0, way)
    for h in range(2):
        for way in (1, -1):
            hop(h, 1, 0, 0, way)
    own_t.wait()
    rows = pl.ds(test_rows(0, 0, 0), TESTS)
    send(tall.at[rows], tall.at[rows], t_sem.at[16], pair)
    own_g.wait()
    for t in range(TILES):
        rows = pl.ds(t * TILE, TILE)
        send(gbuf.at[0, rows], gbuf.at[1, rows], g_sem.at[t], pair)

    mine = (c + z) % 2
    keeps_first = ((z - mine + 4) % 4) // 2 == yh
    kept = jnp.where(keeps_first, 0, 1)

    def tile(s, dx, p, t):
        item = dx * 2 + p
        rows = pl.ds(pl.multiple_of(t * TILE, TILE), TILE)
        acc = jnp.zeros((TILE, 2 * LANES), jnp.float32)
        for h in range(2):
            for k in range(0, HALF, STEP):
                ks = pl.ds(k, STEP)
                pieces = [
                    buf[0, dx, 2 * p + i, ks, :] if h == 0 else buf[1, 2 * p + i, dx, ks, :]
                    for i in range(2)
                ]
                acc += jnp.dot(
                    gbuf[s, rows, pl.ds(h * HALF + k, STEP)],
                    jnp.concatenate(pieces, axis=1),
                    preferred_element_type=jnp.float32,
                )
        cst[s, item, 0, rows, :] = acc[:, :LANES]
        cst[s, item, 1, rows, :] = acc[:, LANES:]

    def to_other_core(s, dx, p):
        item = dx * 2 + p
        send(cst.at[s, item, 1 - mine], xrecv.at[s, item], x_sem.at[s * 8 + item], twin)

    def multiply(s, dx, p):
        def body(t, carry):
            tile(s, dx, p, t)
            return carry

        lax.fori_loop(0, TILES, body, 0)
        to_other_core(s, dx, p)

    given = []
    ways = (pair, diagonal)

    def add_twin(s, dx, p):
        item = dx * 2 + p
        ref = xrecv.at[s, item]
        pltpu.make_async_remote_copy(
            ref, ref, send_sem.at[0], x_sem.at[s * 8 + item], device_id=twin, device_id_type=MESH
        ).wait_recv()
        total = cst[s, item, mine] + xrecv[s, item]
        pst[s, item] = total.astype(jnp.bfloat16)
        keep = kept == p
        if s == 0:
            cst[s, item, mine] = total
            copy = pltpu.make_async_remote_copy(
                pst.at[s, item],
                rcv.at[0, dx],
                send_sem.at[len(sent)],
                rcv_sem.at[dx],
                device_id=opposite,
                device_id_type=MESH,
            )
            sent.append(None)

            @pl.when(jnp.logical_not(keep))
            def _():
                copy.start()

            given.append((copy, keep))
        else:
            slot = jnp.where(keep, 1, 2)
            hi = jnp.where(keep, yh, 1 - yh)
            send(
                pst.at[s, item], rcv.at[slot, dx], rcv_sem.at[slot * 4 + dx],
                (pair[0], hi * 2 + c),
            )

    def finish(dx):
        for k in range(3):
            ref = rcv.at[k, dx]
            pltpu.make_async_remote_copy(
                ref, ref, send_sem.at[0], rcv_sem.at[k * 4 + dx], device_id=twin, device_id_type=MESH
            ).wait_recv()
        chunk = ((x - dx + 4) % 4) * 2
        own = cst[0, dx * 2 + kept, mine] + rcv[0, dx].astype(jnp.float32)
        other = rcv[1, dx].astype(jnp.float32) + rcv[2, dx].astype(jnp.float32)
        lanes = pl.ds(pl.multiple_of((chunk + yl) * LANES, LANES), LANES)
        out_ref[:, lanes] = own.astype(jnp.bfloat16)
        lanes = pl.ds(pl.multiple_of((chunk + 1 - yl) * LANES, LANES), LANES)
        out_ref[:, lanes] = other.astype(jnp.bfloat16)

    def relay_tests(a):
        for h in range(2):
            tests_arrived(h, a, 1)
            tests_arrived(h, a, 3)
            test_hop(h, 1, a, 1, 1, part=0)
            test_hop(h, 1, a, 3, -1, part=1)

    def gradients(t):
        landed(gbuf.at[1, pl.ds(t * TILE, TILE)], g_sem.at[t])

    each(1, 0)
    each(3, 0)
    for h in range(2):
        hop(h, 0, 1, 0, 1, part=0)
        hop(h, 0, 3, 0, -1, part=1)
    for a in (1, 3):
        for h in range(2):
            for way in (1, -1):
                hop(h, 1, a, 0, way)
    each(0, 1)
    each(0, 3)
    for h in range(2):
        hop(h, 1, 0, 1, 1, part=0)
        hop(h, 1, 0, 3, -1, part=1)
    tests_arrived(1, 0, 0)
    for axis in range(2):
        for h in range(2):
            for way in (1, -1):
                test_hop(h, axis, 0, 0, way)
    multiply(0, 0, 0)
    each(2, 0)
    for h in range(2):
        for way in (1, -1):
            hop(h, 1, 2, 0, way)
    add_twin(0, 0, 0)
    for a in (1, 3):
        each(a, 1)
        each(a, 3)
        for h in range(2):
            hop(h, 1, a, 1, 1, part=0)
            hop(h, 1, a, 3, -1, part=1)
        if a == 1:
            multiply(0, 1, 0)
            gradients(0)
            tile(1, 0, 0, 0)
            tile(1, 1, 0, 0)
    for a in (1, 3):
        for h in range(2):
            tests_arrived(h, a, 0)
            tests_arrived(h, 0, a)
            way = 1 if a == 1 else -1
            test_hop(h, 0, a, 0, way, part=a // 2)
            test_hop(h, 1, 0, a, way, part=a // 2)
    add_twin(0, 1, 0)
    multiply(0, 3, 0)
    tile(1, 3, 0, 0)
    each(0, 2)
    multiply(0, 0, 1)
    tile(1, 0, 1, 0)
    add_twin(0, 3, 0)
    each(2, 1)
    each(2, 3)
    for h in range(2):
        hop(h, 1, 2, 1, 1, part=0)
        hop(h, 1, 2, 3, -1, part=1)
    for a in (1, 3):
        for h in range(2):
            for way in (1, -1):
                test_hop(h, 1, a, 0, way)
    add_twin(0, 0, 1)
    each(1, 2)
    multiply(0, 1, 1)
    multiply(0, 2, 0)
    tile(1, 1, 1, 0)
    tile(1, 2, 0, 0)
    add_twin(0, 1, 1)
    add_twin(0, 2, 0)
    for h in range(2):
        tests_arrived(h, 2, 0)
        for way in (1, -1):
            test_hop(h, 1, 2, 0, way)
    gradients(1)
    before = None
    for now in ((0, 0), (0, 1), (1, 0), (1, 1), (3, 0), (2, 0)):
        tile(1, *now, 1)
        to_other_core(1, *now)
        if before is not None:
            add_twin(1, *before)
        before = now
    each(3, 2)
    multiply(0, 3, 1)
    add_twin(1, *before)
    multiply(1, 3, 1)
    add_twin(0, 3, 1)
    add_twin(1, 3, 1)
    finish(0)
    finish(1)
    each(2, 2)
    multiply(0, 2, 1)
    relay_tests(1)
    multiply(1, 2, 1)
    relay_tests(3)
    add_twin(0, 2, 1)
    add_twin(1, 2, 1)
    relay_tests(2)
    finish(3)
    for h in range(2):
        for a in range(4):
            tests_arrived(h, a, 2)
    finish(2)

    def score(quarter, i):
        rows = pl.ds(pl.multiple_of(quarter * 256 + i * LANES, LANES), LANES)
        part_scores[quarter, pl.ds(i * LANES, LANES), :] = lax.dot_general(
            tall[rows, :], out_ref[...], (((1,), (1,)), ((), ())),
            preferred_element_type=jnp.float32,
        )

    def to_twin(quarter, k, i):
        rows = pl.ds(i * LANES, LANES)
        send(
            part_scores.at[quarter, rows], twin_scores.at[k, rows], score_sem.at[k * 2 + i], twin
        )

    def twin_sum(quarter, k, i):
        rows = pl.ds(i * LANES, LANES)
        landed(twin_scores.at[k, rows], score_sem.at[k * 2 + i])
        return part_scores[quarter, rows, :] + twin_scores[k, rows, :]

    far, near = (1 - yh) * 2, yh * 2
    for i in range(2):
        score(far + 1 - c, i)
        to_twin(far + 1 - c, 0, i)
    for i in range(2):
        score(far + c, i)
        part_scores[far + c, pl.ds(i * LANES, LANES), :] = twin_sum(far + c, 0, i)
        for k in range(2):
            rows = pl.ds(i * LANES + k * 64, 64)
            send(
                part_scores.at[far + c, rows], relay_scores.at[i, k],
                score_sem.at[4 + i * 2 + k], ways[i],
            )
    for i in range(2):
        score(near + 1 - c, i)
        to_twin(near + 1 - c, 1, i)
    for k in range(2):
        for i in range(2):
            landed(relay_scores.at[i, k], score_sem.at[4 + i * 2 + k])
            send(
                relay_scores.at[i, k], far_scores.at[i, k], score_sem.at[8 + i * 2 + k],
                ways[1 - i],
            )
        score(near + c, k)
    for i in range(2):
        score_ref[pl.ds(i * LANES, LANES), :] = twin_sum(near + c, 1, i)
    for k in range(2):
        for i in range(2):
            landed(far_scores.at[i, k], score_sem.at[8 + i * 2 + k])
            rows = pl.ds(i * LANES + k * 64, 64)
            score_ref[rows, :] = score_ref[rows, :] + far_scores[i, k]
    for copy in sent:
        if copy is not None:
            copy.wait_send()
    for copy, keep in given:
        @pl.when(jnp.logical_not(keep))
        def _():
            copy.wait_send()


def local(train_grads, projection, test_features, example_weights):
    flops = 2 * 2 * ROWS * DEPTH * 2048
    inner, projected = pl.pallas_call(
        project_kernel,
        out_shape=(
            jax.ShapeDtypeStruct((256, ROWS), jnp.float32),
            jax.ShapeDtypeStruct((ROWS, 1024), jnp.bfloat16),
        ),
        in_specs=[pl.BlockSpec(memory_space=pltpu.HBM)] * 3,
        out_specs=(pl.BlockSpec(memory_space=pltpu.VMEM),) * 2,
        scratch_shapes=[
            pltpu.VMEM((2, 4, 4, HALF, LANES), jnp.bfloat16),
            pltpu.VMEM((2, ROWS, DEPTH), jnp.bfloat16),
            pltpu.VMEM((2, 8, 2, ROWS, LANES), jnp.float32),
            pltpu.VMEM((2, 8, ROWS, LANES), jnp.float32),
            pltpu.VMEM((2, 8, ROWS, LANES), jnp.bfloat16),
            pltpu.VMEM((3, 4, ROWS, LANES), jnp.bfloat16),
            pltpu.VMEM((1024, 1024), jnp.bfloat16),
            pltpu.VMEM((4, 256, ROWS), jnp.float32),
            pltpu.VMEM((2, 256, ROWS), jnp.float32),
            pltpu.VMEM((2, 2, 64, ROWS), jnp.float32),
            pltpu.VMEM((2, 2, 64, ROWS), jnp.float32),
            pltpu.SemaphoreType.DMA((4,)),
            pltpu.SemaphoreType.DMA((160,)),
            pltpu.SemaphoreType.DMA((32,)),
            pltpu.SemaphoreType.DMA((TILES,)),
            pltpu.SemaphoreType.DMA((16,)),
            pltpu.SemaphoreType.DMA((12,)),
            pltpu.SemaphoreType.DMA((32,)),
            pltpu.SemaphoreType.DMA((12,)),
        ],
        compiler_params=pltpu.CompilerParams(
            collective_id=0, has_side_effects=True, vmem_limit_bytes=44 * 1024 * 1024
        ),
        cost_estimate=pl.CostEstimate(
            flops=flops, bytes_accessed=8 * 2**20, transcendentals=0
        ),
    )(*[pltpu.with_memory_space_constraint(v, pltpu.HBM) for v in (train_grads, projection, test_features)])
    return inner * example_weights[None, :], projected


def solution(mesh):
    return jax.shard_map(
        local,
        mesh=mesh,
        in_specs=(P("ex", "feat"), P("feat", "ex"), P("ex", "feat"), P("ex")),
        out_specs=(P("feat", "ex"), P("ex", "feat")),
        check_vma=False,
    )
```

```python
import jax
import jax.numpy as jnp
from jax import lax
from jax.experimental import pallas as pl
from jax.experimental.pallas import tpu as pltpu
from jax.sharding import PartitionSpec as P

MESH = pl.DeviceIdType.MESH
ROWS = 384
TESTS = 32
TILE = 192
TILES = ROWS // TILE
DEPTH = 4096
HALF = DEPTH // 2
QUARTER = HALF // 2
LANES = 128
STEP = 512


def project_kernel(
    g_hbm, r_hbm, t_hbm, score_ref, out_ref, buf, gbuf, cst, xrecv, pst, rcv,
    tall, part_scores, twin_scores, away_scores, relay_scores, far_scores,
    local_sem, send_sem, piece_sem, g_sem, x_sem, rcv_sem, t_sem, score_sem,
):
    ex = lax.axis_index("ex")
    ft = lax.axis_index("feat")
    z, x, yl = ex // 8, (ex // 2) % 4, ex % 2
    yh, c = ft // 2, ft % 2

    def at(dx=0, dz=0, flip_lo=0, flip_hi=0, flip_core=0):
        lo = 1 - yl if flip_lo else yl
        hi = 1 - yh if flip_hi else yh
        core = 1 - c if flip_core else c
        return (((z + dz) % 4) * 8 + ((x + dx) % 4) * 2 + lo, hi * 2 + core)

    first = ("x", "z")
    second = ("z", "x")

    def neighbour(axis, way):
        return at(dx=way) if axis == "x" else at(dz=way)

    pair, twin, opposite, diagonal = (
        at(flip_lo=1), at(flip_core=1), at(flip_hi=1), at(flip_lo=1, flip_hi=1)
    )
    sent = []

    def send(src, dst, sem, device):
        copy = pltpu.make_async_remote_copy(
            src, dst, send_sem.at[len(sent)], sem, device_id=device, device_id_type=MESH
        )
        copy.start()
        sent.append(copy)

    own_r = []
    for h in range(2):
        copy = pltpu.make_async_copy(
            r_hbm.at[pl.ds(h * HALF, HALF)], buf.at[h, 0, 0], local_sem.at[h]
        )
        copy.start()
        own_r.append(copy)
    own_g = pltpu.make_async_copy(g_hbm, gbuf.at[0], local_sem.at[2])
    own_g.start()

    def test_rows(h, a, b):
        dx, dz = (a, b) if h == 0 else (b, a)
        lo = yl if h == 0 else 1 - yl
        source = ((z - dz + 4) % 4) * 8 + ((x - dx + 4) % 4) * 2 + lo
        return pl.multiple_of(source * TESTS, TESTS)

    own_t = pltpu.make_async_copy(
        t_hbm, tall.at[pl.ds(test_rows(0, 0, 0), TESTS)], local_sem.at[3]
    )
    own_t.start()

    barrier = pltpu.get_barrier_semaphore()
    friends = [at(dx=1), at(dx=-1), at(dz=1), at(dz=-1), pair, twin, opposite, diagonal]
    for device in friends:
        pl.semaphore_signal(barrier, inc=1, device_id=device, device_id_type=MESH)
    pl.semaphore_wait(barrier, len(friends))

    def sem_of(h, a, b):
        return piece_sem.at[h * 16 + a * 4 + b]

    def hop(h, axis, a, b, way, part=None):
        if axis == 0:
            a2, b2 = (a + way) % 4, b
        else:
            a2, b2 = a, (b + way) % 4
        src, dst = buf.at[h, a, b], buf.at[h, a2, b2]
        if part is not None:
            rows = pl.ds(part * QUARTER, QUARTER)
            src, dst = src.at[rows], dst.at[rows]
        send(src, dst, sem_of(h, a2, b2), neighbour((first, second)[axis][h], way))

    def arrived(h, a, b):
        ref = buf.at[h, a, b]
        pltpu.make_async_remote_copy(
            ref, ref, send_sem.at[0], sem_of(h, a, b), device_id=twin, device_id_type=MESH
        ).wait_recv()

    def test_hop(h, axis, a, b, way, part=None):
        a2, b2 = ((a + way) % 4, b) if axis == 0 else (a, (b + way) % 4)
        start, count = test_rows(h, a, b), TESTS
        if part is not None:
            start, count = pl.multiple_of(start + part * (TESTS // 2), TESTS // 2), TESTS // 2
        rows = pl.ds(start, count)
        send(
            tall.at[rows], tall.at[rows], t_sem.at[h * 16 + a2 * 4 + b2],
            neighbour((first, second)[axis][h], way),
        )

    def tests_arrived(h, a, b):
        ref = tall.at[pl.ds(test_rows(h, a, b), TESTS)]
        pltpu.make_async_remote_copy(
            ref, ref, send_sem.at[0], t_sem.at[h * 16 + a * 4 + b], device_id=twin,
            device_id_type=MESH,
        ).wait_recv()

    def landed(ref, sem):
        pltpu.make_async_remote_copy(
            ref, ref, send_sem.at[0], sem, device_id=twin, device_id_type=MESH
        ).wait_recv()

    def each(a, b):
        for h in range(2):
            arrived(h, a, b)

    for h in range(2):
        own_r[h].wait()
        for way in (1, -1):
            hop(h, 0, 0, 0, way)
    for h in range(2):
        for way in (1, -1):
            hop(h, 1, 0, 0, way)
    own_t.wait()
    rows = pl.ds(test_rows(0, 0, 0), TESTS)
    send(tall.at[rows], tall.at[rows], t_sem.at[16], pair)
    own_g.wait()
    for t in range(TILES):
        rows = pl.ds(t * TILE, TILE)
        send(gbuf.at[0, rows], gbuf.at[1, rows], g_sem.at[t], pair)

    mine = (c + z) % 2
    keeps_first = ((z - mine + 4) % 4) // 2 == yh
    kept = jnp.where(keeps_first, 0, 1)

    def tile(s, dx, p, t):
        item = dx * 2 + p
        rows = pl.ds(pl.multiple_of(t * TILE, TILE), TILE)
        acc = jnp.zeros((TILE, 2 * LANES), jnp.float32)
        for h in range(2):
            for k in range(0, HALF, STEP):
                ks = pl.ds(k, STEP)
                pieces = [
                    buf[0, dx, 2 * p + i, ks, :] if h == 0 else buf[1, 2 * p + i, dx, ks, :]
                    for i in range(2)
                ]
                acc += jnp.dot(
                    gbuf[s, rows, pl.ds(h * HALF + k, STEP)],
                    jnp.concatenate(pieces, axis=1),
                    preferred_element_type=jnp.float32,
                )
        cst[s, item, 0, rows, :] = acc[:, :LANES]
        cst[s, item, 1, rows, :] = acc[:, LANES:]

    def to_other_core(s, dx, p):
        item = dx * 2 + p
        send(cst.at[s, item, 1 - mine], xrecv.at[s, item], x_sem.at[s * 8 + item], twin)

    def multiply(s, dx, p):
        def body(t, carry):
            tile(s, dx, p, t)
            return carry

        lax.fori_loop(0, TILES, body, 0)
        to_other_core(s, dx, p)

    given = []
    ways = (pair, diagonal)

    def add_twin(s, dx, p):
        item = dx * 2 + p
        ref = xrecv.at[s, item]
        pltpu.make_async_remote_copy(
            ref, ref, send_sem.at[0], x_sem.at[s * 8 + item], device_id=twin, device_id_type=MESH
        ).wait_recv()
        total = cst[s, item, mine] + xrecv[s, item]
        pst[s, item] = total.astype(jnp.bfloat16)
        keep = kept == p
        if s == 0:
            cst[s, item, mine] = total
            copy = pltpu.make_async_remote_copy(
                pst.at[s, item],
                rcv.at[0, dx],
                send_sem.at[len(sent)],
                rcv_sem.at[dx],
                device_id=opposite,
                device_id_type=MESH,
            )
            sent.append(None)

            @pl.when(jnp.logical_not(keep))
            def _():
                copy.start()

            given.append((copy, keep))
        else:
            slot = jnp.where(keep, 1, 2)
            hi = jnp.where(keep, yh, 1 - yh)
            send(
                pst.at[s, item], rcv.at[slot, dx], rcv_sem.at[slot * 4 + dx],
                (pair[0], hi * 2 + c),
            )

    def finish(dx):
        for k in range(3):
            ref = rcv.at[k, dx]
            pltpu.make_async_remote_copy(
                ref, ref, send_sem.at[0], rcv_sem.at[k * 4 + dx], device_id=twin, device_id_type=MESH
            ).wait_recv()
        chunk = ((x - dx + 4) % 4) * 2
        own = cst[0, dx * 2 + kept, mine] + rcv[0, dx].astype(jnp.float32)
        other = rcv[1, dx].astype(jnp.float32) + rcv[2, dx].astype(jnp.float32)
        lanes = pl.ds(pl.multiple_of((chunk + yl) * LANES, LANES), LANES)
        out_ref[:, lanes] = own.astype(jnp.bfloat16)
        lanes = pl.ds(pl.multiple_of((chunk + 1 - yl) * LANES, LANES), LANES)
        out_ref[:, lanes] = other.astype(jnp.bfloat16)

    def relay_tests(a):
        for h in range(2):
            tests_arrived(h, a, 1)
            tests_arrived(h, a, 3)
            test_hop(h, 1, a, 1, 1, part=0)
            test_hop(h, 1, a, 3, -1, part=1)

    def gradients(t):
        landed(gbuf.at[1, pl.ds(t * TILE, TILE)], g_sem.at[t])

    each(1, 0)
    each(3, 0)
    for h in range(2):
        hop(h, 0, 1, 0, 1, part=0)
        hop(h, 0, 3, 0, -1, part=1)
    for a in (1, 3):
        for h in range(2):
            for way in (1, -1):
                hop(h, 1, a, 0, way)
    each(0, 1)
    each(0, 3)
    for h in range(2):
        hop(h, 1, 0, 1, 1, part=0)
        hop(h, 1, 0, 3, -1, part=1)
    tests_arrived(1, 0, 0)
    for axis in range(2):
        for h in range(2):
            for way in (1, -1):
                test_hop(h, axis, 0, 0, way)
    multiply(0, 0, 0)
    each(2, 0)
    for h in range(2):
        for way in (1, -1):
            hop(h, 1, 2, 0, way)
    add_twin(0, 0, 0)
    for a in (1, 3):
        each(a, 1)
        each(a, 3)
        for h in range(2):
            hop(h, 1, a, 1, 1, part=0)
            hop(h, 1, a, 3, -1, part=1)
        if a == 1:
            multiply(0, 1, 0)
            gradients(0)
            tile(1, 0, 0, 0)
            tile(1, 1, 0, 0)
    for a in (1, 3):
        for h in range(2):
            tests_arrived(h, a, 0)
            tests_arrived(h, 0, a)
            way = 1 if a == 1 else -1
            test_hop(h, 0, a, 0, way, part=a // 2)
            test_hop(h, 1, 0, a, way, part=a // 2)
    add_twin(0, 1, 0)
    multiply(0, 3, 0)
    tile(1, 3, 0, 0)
    each(0, 2)
    multiply(0, 0, 1)
    tile(1, 0, 1, 0)
    add_twin(0, 3, 0)
    each(2, 1)
    each(2, 3)
    for h in range(2):
        hop(h, 1, 2, 1, 1, part=0)
        hop(h, 1, 2, 3, -1, part=1)
    for a in (1, 3):
        for h in range(2):
            for way in (1, -1):
                test_hop(h, 1, a, 0, way)
    add_twin(0, 0, 1)
    each(1, 2)
    multiply(0, 1, 1)
    multiply(0, 2, 0)
    tile(1, 1, 1, 0)
    tile(1, 2, 0, 0)
    add_twin(0, 1, 1)
    add_twin(0, 2, 0)
    for h in range(2):
        tests_arrived(h, 2, 0)
        for way in (1, -1):
            test_hop(h, 1, 2, 0, way)
    gradients(1)
    before = None
    for now in ((0, 0), (0, 1), (1, 0), (1, 1), (3, 0), (2, 0)):
        tile(1, *now, 1)
        to_other_core(1, *now)
        if before is not None:
            add_twin(1, *before)
        before = now
    each(3, 2)
    multiply(0, 3, 1)
    add_twin(1, *before)
    multiply(1, 3, 1)
    add_twin(0, 3, 1)
    add_twin(1, 3, 1)
    finish(0)
    finish(1)
    each(2, 2)
    multiply(0, 2, 1)
    relay_tests(1)
    multiply(1, 2, 1)
    relay_tests(3)
    add_twin(0, 2, 1)
    add_twin(1, 2, 1)
    relay_tests(2)
    finish(3)
    for h in range(2):
        for a in range(4):
            tests_arrived(h, a, 2)
    finish(2)

    def score(quarter, i):
        rows = pl.ds(pl.multiple_of(quarter * 256 + i * LANES, LANES), LANES)
        part_scores[quarter, pl.ds(i * LANES, LANES), :] = lax.dot_general(
            tall[rows, :], out_ref[...], (((1,), (1,)), ((), ())),
            preferred_element_type=jnp.float32,
        )

    def to_twin(quarter, k, i):
        rows = pl.ds(i * LANES, LANES)
        send(
            part_scores.at[quarter, rows], twin_scores.at[k, rows], score_sem.at[k * 2 + i], twin
        )

    def twin_sum(quarter, k, i):
        rows = pl.ds(i * LANES, LANES)
        landed(twin_scores.at[k, rows], score_sem.at[k * 2 + i])
        return part_scores[quarter, rows, :] + twin_scores[k, rows, :]

    far, near = (1 - yh) * 2, yh * 2
    for i in range(2):
        score(far + 1 - c, i)
        to_twin(far + 1 - c, 0, i)
    for i in range(2):
        score(far + c, i)
        total = twin_sum(far + c, 0, i).astype(jnp.bfloat16)
        for k in range(2):
            away_scores[i, k] = total[k * 64 : k * 64 + 64]
        for k in range(2):
            send(
                away_scores.at[i, k], relay_scores.at[i, k],
                score_sem.at[4 + i * 2 + k], ways[i],
            )
    for i in range(2):
        score(near + 1 - c, i)
        to_twin(near + 1 - c, 1, i)
    for k in range(2):
        for i in range(2):
            landed(relay_scores.at[i, k], score_sem.at[4 + i * 2 + k])
            send(
                relay_scores.at[i, k], far_scores.at[i, k], score_sem.at[8 + i * 2 + k],
                ways[1 - i],
            )
        score(near + c, k)
    for i in range(2):
        score_ref[pl.ds(i * LANES, LANES), :] = twin_sum(near + c, 1, i)
    for k in range(2):
        for i in range(2):
            landed(far_scores.at[i, k], score_sem.at[8 + i * 2 + k])
            rows = pl.ds(i * LANES + k * 64, 64)
            score_ref[rows, :] = score_ref[rows, :] + far_scores[i, k].astype(jnp.float32)
    for copy in sent:
        if copy is not None:
            copy.wait_send()
    for copy, keep in given:
        @pl.when(jnp.logical_not(keep))
        def _():
            copy.wait_send()


def local(train_grads, projection, test_features, example_weights):
    flops = 2 * 2 * ROWS * DEPTH * 2048
    inner, projected = pl.pallas_call(
        project_kernel,
        out_shape=(
            jax.ShapeDtypeStruct((256, ROWS), jnp.float32),
            jax.ShapeDtypeStruct((ROWS, 1024), jnp.bfloat16),
        ),
        in_specs=[pl.BlockSpec(memory_space=pltpu.HBM)] * 3,
        out_specs=(pl.BlockSpec(memory_space=pltpu.VMEM),) * 2,
        scratch_shapes=[
            pltpu.VMEM((2, 4, 4, HALF, LANES), jnp.bfloat16),
            pltpu.VMEM((2, ROWS, DEPTH), jnp.bfloat16),
            pltpu.VMEM((2, 8, 2, ROWS, LANES), jnp.float32),
            pltpu.VMEM((2, 8, ROWS, LANES), jnp.float32),
            pltpu.VMEM((2, 8, ROWS, LANES), jnp.bfloat16),
            pltpu.VMEM((3, 4, ROWS, LANES), jnp.bfloat16),
            pltpu.VMEM((1024, 1024), jnp.bfloat16),
            pltpu.VMEM((4, 256, ROWS), jnp.float32),
            pltpu.VMEM((2, 256, ROWS), jnp.float32),
            pltpu.VMEM((2, 2, 64, ROWS), jnp.bfloat16),
            pltpu.VMEM((2, 2, 64, ROWS), jnp.bfloat16),
            pltpu.VMEM((2, 2, 64, ROWS), jnp.bfloat16),
            pltpu.SemaphoreType.DMA((4,)),
            pltpu.SemaphoreType.DMA((160,)),
            pltpu.SemaphoreType.DMA((32,)),
            pltpu.SemaphoreType.DMA((TILES,)),
            pltpu.SemaphoreType.DMA((16,)),
            pltpu.SemaphoreType.DMA((12,)),
            pltpu.SemaphoreType.DMA((32,)),
            pltpu.SemaphoreType.DMA((12,)),
        ],
        compiler_params=pltpu.CompilerParams(
            collective_id=0, has_side_effects=True, vmem_limit_bytes=44 * 1024 * 1024
        ),
        cost_estimate=pl.CostEstimate(
            flops=flops, bytes_accessed=8 * 2**20, transcendentals=0
        ),
    )(*[pltpu.with_memory_space_constraint(v, pltpu.HBM) for v in (train_grads, projection, test_features)])
    return inner * example_weights[None, :], projected


def solution(mesh):
    return jax.shard_map(
        local,
        mesh=mesh,
        in_specs=(P("ex", "feat"), P("feat", "ex"), P("ex", "feat"), P("ex")),
        out_specs=(P("feat", "ex"), P("ex", "feat")),
        check_vma=False,
    )
```

```python
import jax
import jax.numpy as jnp
from jax import lax
from jax.experimental import pallas as pl
from jax.experimental.pallas import tpu as pltpu
from jax.sharding import PartitionSpec as P

MESH = pl.DeviceIdType.MESH
ROWS = 384
TESTS = 32
TILE = 192
TILES = ROWS // TILE
DEPTH = 4096
HALF = DEPTH // 2
QUARTER = HALF // 2
LANES = 128
STEP = 512


def project_kernel(
    g_hbm, r_hbm, t_hbm, score_ref, out_ref, buf, gbuf, cst, xrecv, pst, rcv,
    tall, turned, part_scores, twin_scores, away_scores, relay_scores, far_scores,
    local_sem, send_sem, piece_sem, g_sem, x_sem, rcv_sem, t_sem, score_sem,
):
    ex = lax.axis_index("ex")
    ft = lax.axis_index("feat")
    z, x, yl = ex // 8, (ex // 2) % 4, ex % 2
    yh, c = ft // 2, ft % 2

    def at(dx=0, dz=0, flip_lo=0, flip_hi=0, flip_core=0):
        lo = 1 - yl if flip_lo else yl
        hi = 1 - yh if flip_hi else yh
        core = 1 - c if flip_core else c
        return (((z + dz) % 4) * 8 + ((x + dx) % 4) * 2 + lo, hi * 2 + core)

    first = ("x", "z")
    second = ("z", "x")

    def neighbour(axis, way):
        return at(dx=way) if axis == "x" else at(dz=way)

    pair, twin, opposite, diagonal = (
        at(flip_lo=1), at(flip_core=1), at(flip_hi=1), at(flip_lo=1, flip_hi=1)
    )
    sent = []

    def send(src, dst, sem, device):
        copy = pltpu.make_async_remote_copy(
            src, dst, send_sem.at[len(sent)], sem, device_id=device, device_id_type=MESH
        )
        copy.start()
        sent.append(copy)

    own_r = []
    for h in range(2):
        copy = pltpu.make_async_copy(
            r_hbm.at[pl.ds(h * HALF, HALF)], buf.at[h, 0, 0], local_sem.at[h]
        )
        copy.start()
        own_r.append(copy)
    own_g = pltpu.make_async_copy(g_hbm, gbuf.at[0], local_sem.at[2])
    own_g.start()

    def test_rows(h, a, b):
        dx, dz = (a, b) if h == 0 else (b, a)
        lo = yl if h == 0 else 1 - yl
        source = ((z - dz + 4) % 4) * 8 + ((x - dx + 4) % 4) * 2 + lo
        return pl.multiple_of(source * TESTS, TESTS)

    own_t = pltpu.make_async_copy(
        t_hbm, tall.at[pl.ds(test_rows(0, 0, 0), TESTS)], local_sem.at[3]
    )
    own_t.start()

    barrier = pltpu.get_barrier_semaphore()
    friends = [at(dx=1), at(dx=-1), at(dz=1), at(dz=-1), pair, twin, opposite, diagonal]
    for device in friends:
        pl.semaphore_signal(barrier, inc=1, device_id=device, device_id_type=MESH)
    pl.semaphore_wait(barrier, len(friends))

    def sem_of(h, a, b):
        return piece_sem.at[h * 16 + a * 4 + b]

    def hop(h, axis, a, b, way, part=None):
        if axis == 0:
            a2, b2 = (a + way) % 4, b
        else:
            a2, b2 = a, (b + way) % 4
        src, dst = buf.at[h, a, b], buf.at[h, a2, b2]
        if part is not None:
            rows = pl.ds(part * QUARTER, QUARTER)
            src, dst = src.at[rows], dst.at[rows]
        send(src, dst, sem_of(h, a2, b2), neighbour((first, second)[axis][h], way))

    def arrived(h, a, b):
        ref = buf.at[h, a, b]
        pltpu.make_async_remote_copy(
            ref, ref, send_sem.at[0], sem_of(h, a, b), device_id=twin, device_id_type=MESH
        ).wait_recv()

    def test_hop(h, axis, a, b, way, part=None):
        a2, b2 = ((a + way) % 4, b) if axis == 0 else (a, (b + way) % 4)
        start, count = test_rows(h, a, b), TESTS
        if part is not None:
            start, count = pl.multiple_of(start + part * (TESTS // 2), TESTS // 2), TESTS // 2
        rows = pl.ds(start, count)
        send(
            tall.at[rows], tall.at[rows], t_sem.at[h * 16 + a2 * 4 + b2],
            neighbour((first, second)[axis][h], way),
        )

    def tests_arrived(h, a, b):
        ref = tall.at[pl.ds(test_rows(h, a, b), TESTS)]
        pltpu.make_async_remote_copy(
            ref, ref, send_sem.at[0], t_sem.at[h * 16 + a * 4 + b], device_id=twin,
            device_id_type=MESH,
        ).wait_recv()

    def landed(ref, sem):
        pltpu.make_async_remote_copy(
            ref, ref, send_sem.at[0], sem, device_id=twin, device_id_type=MESH
        ).wait_recv()

    def each(a, b):
        for h in range(2):
            arrived(h, a, b)

    for h in range(2):
        own_r[h].wait()
        for way in (1, -1):
            hop(h, 0, 0, 0, way)
    for h in range(2):
        for way in (1, -1):
            hop(h, 1, 0, 0, way)
    own_t.wait()
    rows = pl.ds(test_rows(0, 0, 0), TESTS)
    send(tall.at[rows], tall.at[rows], t_sem.at[16], pair)
    own_g.wait()
    for t in range(TILES):
        rows = pl.ds(t * TILE, TILE)
        send(gbuf.at[0, rows], gbuf.at[1, rows], g_sem.at[t], pair)

    mine = (c + z) % 2
    keeps_first = ((z - mine + 4) % 4) // 2 == yh
    kept = jnp.where(keeps_first, 0, 1)

    def tile(s, dx, p, t):
        item = dx * 2 + p
        rows = pl.ds(pl.multiple_of(t * TILE, TILE), TILE)
        acc = jnp.zeros((TILE, 2 * LANES), jnp.float32)
        for h in range(2):
            for k in range(0, HALF, STEP):
                ks = pl.ds(k, STEP)
                pieces = [
                    buf[0, dx, 2 * p + i, ks, :] if h == 0 else buf[1, 2 * p + i, dx, ks, :]
                    for i in range(2)
                ]
                acc += jnp.dot(
                    gbuf[s, rows, pl.ds(h * HALF + k, STEP)],
                    jnp.concatenate(pieces, axis=1),
                    preferred_element_type=jnp.float32,
                )
        cst[s, item, 0, rows, :] = acc[:, :LANES]
        cst[s, item, 1, rows, :] = acc[:, LANES:]

    def to_other_core(s, dx, p):
        item = dx * 2 + p
        send(cst.at[s, item, 1 - mine], xrecv.at[s, item], x_sem.at[s * 8 + item], twin)

    def multiply(s, dx, p):
        def body(t, carry):
            tile(s, dx, p, t)
            return carry

        lax.fori_loop(0, TILES, body, 0)
        to_other_core(s, dx, p)

    given = []
    ways = (pair, diagonal)

    def add_twin(s, dx, p):
        item = dx * 2 + p
        ref = xrecv.at[s, item]
        pltpu.make_async_remote_copy(
            ref, ref, send_sem.at[0], x_sem.at[s * 8 + item], device_id=twin, device_id_type=MESH
        ).wait_recv()
        total = cst[s, item, mine] + xrecv[s, item]
        pst[s, item] = total.astype(jnp.bfloat16)
        keep = kept == p
        if s == 0:
            cst[s, item, mine] = total
            copy = pltpu.make_async_remote_copy(
                pst.at[s, item],
                rcv.at[0, dx],
                send_sem.at[len(sent)],
                rcv_sem.at[dx],
                device_id=opposite,
                device_id_type=MESH,
            )
            sent.append(None)

            @pl.when(jnp.logical_not(keep))
            def _():
                copy.start()

            given.append((copy, keep))
        else:
            slot = jnp.where(keep, 1, 2)
            hi = jnp.where(keep, yh, 1 - yh)
            send(
                pst.at[s, item], rcv.at[slot, dx], rcv_sem.at[slot * 4 + dx],
                (pair[0], hi * 2 + c),
            )

    def finish(dx):
        for k in range(3):
            ref = rcv.at[k, dx]
            pltpu.make_async_remote_copy(
                ref, ref, send_sem.at[0], rcv_sem.at[k * 4 + dx], device_id=twin, device_id_type=MESH
            ).wait_recv()
        chunk = ((x - dx + 4) % 4) * 2
        own = cst[0, dx * 2 + kept, mine] + rcv[0, dx].astype(jnp.float32)
        other = rcv[1, dx].astype(jnp.float32) + rcv[2, dx].astype(jnp.float32)
        lanes = pl.ds(pl.multiple_of((chunk + yl) * LANES, LANES), LANES)
        out_ref[:, lanes] = own.astype(jnp.bfloat16)
        turned[lanes, :] = own.T.astype(jnp.bfloat16)
        lanes = pl.ds(pl.multiple_of((chunk + 1 - yl) * LANES, LANES), LANES)
        out_ref[:, lanes] = other.astype(jnp.bfloat16)
        turned[lanes, :] = other.T.astype(jnp.bfloat16)

    def relay_tests(a):
        for h in range(2):
            tests_arrived(h, a, 1)
            tests_arrived(h, a, 3)
            test_hop(h, 1, a, 1, 1, part=0)
            test_hop(h, 1, a, 3, -1, part=1)

    def gradients(t):
        landed(gbuf.at[1, pl.ds(t * TILE, TILE)], g_sem.at[t])

    each(1, 0)
    each(3, 0)
    for h in range(2):
        hop(h, 0, 1, 0, 1, part=0)
        hop(h, 0, 3, 0, -1, part=1)
    for a in (1, 3):
        for h in range(2):
            for way in (1, -1):
                hop(h, 1, a, 0, way)
    each(0, 1)
    each(0, 3)
    for h in range(2):
        hop(h, 1, 0, 1, 1, part=0)
        hop(h, 1, 0, 3, -1, part=1)
    tests_arrived(1, 0, 0)
    for axis in range(2):
        for h in range(2):
            for way in (1, -1):
                test_hop(h, axis, 0, 0, way)
    multiply(0, 0, 0)
    each(2, 0)
    for h in range(2):
        for way in (1, -1):
            hop(h, 1, 2, 0, way)
    add_twin(0, 0, 0)
    for a in (1, 3):
        each(a, 1)
        each(a, 3)
        for h in range(2):
            hop(h, 1, a, 1, 1, part=0)
            hop(h, 1, a, 3, -1, part=1)
        if a == 1:
            multiply(0, 1, 0)
            gradients(0)
            tile(1, 0, 0, 0)
            tile(1, 1, 0, 0)
    for a in (1, 3):
        for h in range(2):
            tests_arrived(h, a, 0)
            tests_arrived(h, 0, a)
            way = 1 if a == 1 else -1
            test_hop(h, 0, a, 0, way, part=a // 2)
            test_hop(h, 1, 0, a, way, part=a // 2)
    add_twin(0, 1, 0)
    multiply(0, 3, 0)
    tile(1, 3, 0, 0)
    each(0, 2)
    multiply(0, 0, 1)
    tile(1, 0, 1, 0)
    add_twin(0, 3, 0)
    each(2, 1)
    each(2, 3)
    for h in range(2):
        hop(h, 1, 2, 1, 1, part=0)
        hop(h, 1, 2, 3, -1, part=1)
    for a in (1, 3):
        for h in range(2):
            for way in (1, -1):
                test_hop(h, 1, a, 0, way)
    add_twin(0, 0, 1)
    each(1, 2)
    multiply(0, 1, 1)
    multiply(0, 2, 0)
    tile(1, 1, 1, 0)
    tile(1, 2, 0, 0)
    add_twin(0, 1, 1)
    add_twin(0, 2, 0)
    for h in range(2):
        tests_arrived(h, 2, 0)
        for way in (1, -1):
            test_hop(h, 1, 2, 0, way)
    gradients(1)
    before = None
    for now in ((0, 0), (0, 1), (1, 0), (1, 1), (3, 0), (2, 0)):
        tile(1, *now, 1)
        to_other_core(1, *now)
        if before is not None:
            add_twin(1, *before)
        before = now
    each(3, 2)
    multiply(0, 3, 1)
    add_twin(1, *before)
    multiply(1, 3, 1)
    add_twin(0, 3, 1)
    add_twin(1, 3, 1)
    each(2, 2)
    multiply(0, 2, 1)
    relay_tests(1)
    multiply(1, 2, 1)
    relay_tests(3)
    add_twin(0, 2, 1)
    add_twin(1, 2, 1)
    relay_tests(2)
    finish(0)
    finish(1)
    finish(3)
    for h in range(2):
        for a in range(4):
            tests_arrived(h, a, 2)
    finish(2)

    def score(quarter, i):
        rows = pl.ds(pl.multiple_of(quarter * 256 + i * LANES, LANES), LANES)
        part_scores[quarter, pl.ds(i * LANES, LANES), :] = jnp.dot(
            tall[rows, :], turned[...], preferred_element_type=jnp.float32
        )

    def to_twin(quarter, k, i):
        rows = pl.ds(i * LANES, LANES)
        send(
            part_scores.at[quarter, rows], twin_scores.at[k, rows], score_sem.at[k * 2 + i], twin
        )

    def twin_sum(quarter, k, i):
        rows = pl.ds(i * LANES, LANES)
        landed(twin_scores.at[k, rows], score_sem.at[k * 2 + i])
        return part_scores[quarter, rows, :] + twin_scores[k, rows, :]

    far, near = (1 - yh) * 2, yh * 2
    for i in range(2):
        score(far + 1 - c, i)
        to_twin(far + 1 - c, 0, i)
    for i in range(2):
        score(far + c, i)
        total = twin_sum(far + c, 0, i).astype(jnp.bfloat16)
        for k in range(2):
            away_scores[i, k] = total[k * 64 : k * 64 + 64]
        for k in range(2):
            send(
                away_scores.at[i, k], relay_scores.at[i, k],
                score_sem.at[4 + i * 2 + k], ways[i],
            )
    for i in range(2):
        score(near + 1 - c, i)
        to_twin(near + 1 - c, 1, i)
    for k in range(2):
        for i in range(2):
            landed(relay_scores.at[i, k], score_sem.at[4 + i * 2 + k])
            send(
                relay_scores.at[i, k], far_scores.at[i, k], score_sem.at[8 + i * 2 + k],
                ways[1 - i],
            )
        score(near + c, k)
    for i in range(2):
        score_ref[pl.ds(i * LANES, LANES), :] = twin_sum(near + c, 1, i)
    for k in range(2):
        for i in range(2):
            landed(far_scores.at[i, k], score_sem.at[8 + i * 2 + k])
            rows = pl.ds(i * LANES + k * 64, 64)
            score_ref[rows, :] = score_ref[rows, :] + far_scores[i, k].astype(jnp.float32)
    for copy in sent:
        if copy is not None:
            copy.wait_send()
    for copy, keep in given:
        @pl.when(jnp.logical_not(keep))
        def _():
            copy.wait_send()


def local(train_grads, projection, test_features, example_weights):
    flops = 2 * 2 * ROWS * DEPTH * 2048
    inner, projected = pl.pallas_call(
        project_kernel,
        out_shape=(
            jax.ShapeDtypeStruct((256, ROWS), jnp.float32),
            jax.ShapeDtypeStruct((ROWS, 1024), jnp.bfloat16),
        ),
        in_specs=[pl.BlockSpec(memory_space=pltpu.HBM)] * 3,
        out_specs=(pl.BlockSpec(memory_space=pltpu.VMEM),) * 2,
        scratch_shapes=[
            pltpu.VMEM((2, 4, 4, HALF, LANES), jnp.bfloat16),
            pltpu.VMEM((2, ROWS, DEPTH), jnp.bfloat16),
            pltpu.VMEM((2, 8, 2, ROWS, LANES), jnp.float32),
            pltpu.VMEM((2, 8, ROWS, LANES), jnp.float32),
            pltpu.VMEM((2, 8, ROWS, LANES), jnp.bfloat16),
            pltpu.VMEM((3, 4, ROWS, LANES), jnp.bfloat16),
            pltpu.VMEM((1024, 1024), jnp.bfloat16),
            pltpu.VMEM((1024, ROWS), jnp.bfloat16),
            pltpu.VMEM((4, 256, ROWS), jnp.float32),
            pltpu.VMEM((2, 256, ROWS), jnp.float32),
            pltpu.VMEM((2, 2, 64, ROWS), jnp.bfloat16),
            pltpu.VMEM((2, 2, 64, ROWS), jnp.bfloat16),
            pltpu.VMEM((2, 2, 64, ROWS), jnp.bfloat16),
            pltpu.SemaphoreType.DMA((4,)),
            pltpu.SemaphoreType.DMA((160,)),
            pltpu.SemaphoreType.DMA((32,)),
            pltpu.SemaphoreType.DMA((TILES,)),
            pltpu.SemaphoreType.DMA((16,)),
            pltpu.SemaphoreType.DMA((12,)),
            pltpu.SemaphoreType.DMA((32,)),
            pltpu.SemaphoreType.DMA((12,)),
        ],
        compiler_params=pltpu.CompilerParams(
            collective_id=0, has_side_effects=True, vmem_limit_bytes=44 * 1024 * 1024
        ),
        cost_estimate=pl.CostEstimate(
            flops=flops, bytes_accessed=8 * 2**20, transcendentals=0
        ),
    )(*[pltpu.with_memory_space_constraint(v, pltpu.HBM) for v in (train_grads, projection, test_features)])
    return inner * example_weights[None, :], projected


def solution(mesh):
    return jax.shard_map(
        local,
        mesh=mesh,
        in_specs=(P("ex", "feat"), P("feat", "ex"), P("ex", "feat"), P("ex")),
        out_specs=(P("feat", "ex"), P("ex", "feat")),
        check_vma=False,
    )
```

```python
import jax
import jax.numpy as jnp
from jax import lax
from jax.experimental import pallas as pl
from jax.experimental.pallas import tpu as pltpu
from jax.sharding import PartitionSpec as P

MESH = pl.DeviceIdType.MESH
ROWS = 384
TESTS = 32
TILE = 192
TILES = ROWS // TILE
DEPTH = 4096
HALF = DEPTH // 2
QUARTER = HALF // 2
LANES = 128
STEP = 512


def project_kernel(
    g_hbm, r_hbm, t_hbm, score_ref, out_ref, buf, gbuf, cst, xrecv, pst, rcv,
    tall, turned, part_scores, twin_scores, away_scores, relay_scores, far_scores,
    local_sem, send_sem, piece_sem, g_sem, x_sem, rcv_sem, t_sem, score_sem,
):
    ex = lax.axis_index("ex")
    ft = lax.axis_index("feat")
    z, x, yl = ex // 8, (ex // 2) % 4, ex % 2
    yh, c = ft // 2, ft % 2

    def at(dx=0, dz=0, flip_lo=0, flip_hi=0, flip_core=0):
        lo = 1 - yl if flip_lo else yl
        hi = 1 - yh if flip_hi else yh
        core = 1 - c if flip_core else c
        return (((z + dz) % 4) * 8 + ((x + dx) % 4) * 2 + lo, hi * 2 + core)

    first = ("x", "z")
    second = ("z", "x")

    def neighbour(axis, way):
        return at(dx=way) if axis == "x" else at(dz=way)

    pair, twin, opposite, diagonal = (
        at(flip_lo=1), at(flip_core=1), at(flip_hi=1), at(flip_lo=1, flip_hi=1)
    )
    sent = []

    def send(src, dst, sem, device):
        copy = pltpu.make_async_remote_copy(
            src, dst, send_sem.at[len(sent)], sem, device_id=device, device_id_type=MESH
        )
        copy.start()
        sent.append(copy)

    own_r = []
    for h in range(2):
        copy = pltpu.make_async_copy(
            r_hbm.at[pl.ds(h * HALF, HALF)], buf.at[h, 0, 0], local_sem.at[h]
        )
        copy.start()
        own_r.append(copy)
    own_g = pltpu.make_async_copy(g_hbm, gbuf.at[0], local_sem.at[2])
    own_g.start()

    def test_rows(h, a, b):
        dx, dz = (a, b) if h == 0 else (b, a)
        lo = yl if h == 0 else 1 - yl
        source = ((z - dz + 4) % 4) * 8 + ((x - dx + 4) % 4) * 2 + lo
        return pl.multiple_of(source * TESTS, TESTS)

    own_t = pltpu.make_async_copy(
        t_hbm, tall.at[pl.ds(test_rows(0, 0, 0), TESTS)], local_sem.at[3]
    )
    own_t.start()

    barrier = pltpu.get_barrier_semaphore()
    friends = [at(dx=1), at(dx=-1), at(dz=1), at(dz=-1), pair, twin, opposite, diagonal]
    for device in friends:
        pl.semaphore_signal(barrier, inc=1, device_id=device, device_id_type=MESH)
    pl.semaphore_wait(barrier, len(friends))

    def sem_of(h, a, b):
        return piece_sem.at[h * 16 + a * 4 + b]

    def hop(h, axis, a, b, way, part=None):
        if axis == 0:
            a2, b2 = (a + way) % 4, b
        else:
            a2, b2 = a, (b + way) % 4
        src, dst = buf.at[h, a, b], buf.at[h, a2, b2]
        if part is not None:
            rows = pl.ds(part * QUARTER, QUARTER)
            src, dst = src.at[rows], dst.at[rows]
        send(src, dst, sem_of(h, a2, b2), neighbour((first, second)[axis][h], way))

    def arrived(h, a, b):
        ref = buf.at[h, a, b]
        pltpu.make_async_remote_copy(
            ref, ref, send_sem.at[0], sem_of(h, a, b), device_id=twin, device_id_type=MESH
        ).wait_recv()

    def test_hop(h, axis, a, b, way, part=None):
        a2, b2 = ((a + way) % 4, b) if axis == 0 else (a, (b + way) % 4)
        start, count = test_rows(h, a, b), TESTS
        if part is not None:
            start, count = pl.multiple_of(start + part * (TESTS // 2), TESTS // 2), TESTS // 2
        rows = pl.ds(start, count)
        send(
            tall.at[rows], tall.at[rows], t_sem.at[h * 16 + a2 * 4 + b2],
            neighbour((first, second)[axis][h], way),
        )

    def tests_arrived(h, a, b):
        ref = tall.at[pl.ds(test_rows(h, a, b), TESTS)]
        pltpu.make_async_remote_copy(
            ref, ref, send_sem.at[0], t_sem.at[h * 16 + a * 4 + b], device_id=twin,
            device_id_type=MESH,
        ).wait_recv()

    def landed(ref, sem):
        pltpu.make_async_remote_copy(
            ref, ref, send_sem.at[0], sem, device_id=twin, device_id_type=MESH
        ).wait_recv()

    def each(a, b):
        for h in range(2):
            arrived(h, a, b)

    for h in range(2):
        own_r[h].wait()
        for way in (1, -1):
            hop(h, 0, 0, 0, way)
    for h in range(2):
        for way in (1, -1):
            hop(h, 1, 0, 0, way)
    own_t.wait()
    rows = pl.ds(test_rows(0, 0, 0), TESTS)
    send(tall.at[rows], tall.at[rows], t_sem.at[16], pair)
    own_g.wait()
    for t in range(TILES):
        rows = pl.ds(t * TILE, TILE)
        send(gbuf.at[0, rows], gbuf.at[1, rows], g_sem.at[t], pair)

    mine = (c + z) % 2
    keeps_first = ((z - mine + 4) % 4) // 2 == yh
    kept = jnp.where(keeps_first, 0, 1)

    def tile(s, dx, p, t):
        item = dx * 2 + p
        rows = pl.ds(pl.multiple_of(t * TILE, TILE), TILE)
        acc = jnp.zeros((TILE, 2 * LANES), jnp.float32)
        for h in range(2):
            for k in range(0, HALF, STEP):
                ks = pl.ds(k, STEP)
                pieces = [
                    buf[0, dx, 2 * p + i, ks, :] if h == 0 else buf[1, 2 * p + i, dx, ks, :]
                    for i in range(2)
                ]
                acc += jnp.dot(
                    gbuf[s, rows, pl.ds(h * HALF + k, STEP)],
                    jnp.concatenate(pieces, axis=1),
                    preferred_element_type=jnp.float32,
                )
        cst[s, item, 0, rows, :] = acc[:, :LANES]
        cst[s, item, 1, rows, :] = acc[:, LANES:]

    def to_other_core(s, dx, p):
        item = dx * 2 + p
        send(cst.at[s, item, 1 - mine], xrecv.at[s, item], x_sem.at[s * 8 + item], twin)

    def multiply(s, dx, p):
        def body(t, carry):
            tile(s, dx, p, t)
            return carry

        lax.fori_loop(0, TILES, body, 0)
        to_other_core(s, dx, p)

    given = []
    ways = (pair, diagonal)

    def add_twin(s, dx, p):
        item = dx * 2 + p
        ref = xrecv.at[s, item]
        pltpu.make_async_remote_copy(
            ref, ref, send_sem.at[0], x_sem.at[s * 8 + item], device_id=twin, device_id_type=MESH
        ).wait_recv()
        total = cst[s, item, mine] + xrecv[s, item]
        pst[s, item] = total.astype(jnp.bfloat16)
        keep = kept == p
        if s == 0:
            cst[s, item, mine] = total
            copy = pltpu.make_async_remote_copy(
                pst.at[s, item],
                rcv.at[0, dx],
                send_sem.at[len(sent)],
                rcv_sem.at[dx],
                device_id=opposite,
                device_id_type=MESH,
            )
            sent.append(None)

            @pl.when(jnp.logical_not(keep))
            def _():
                copy.start()

            given.append((copy, keep))
        else:
            slot = jnp.where(keep, 1, 2)
            hi = jnp.where(keep, yh, 1 - yh)
            send(
                pst.at[s, item], rcv.at[slot, dx], rcv_sem.at[slot * 4 + dx],
                (pair[0], hi * 2 + c),
            )

    def finish(dx):
        for k in range(3):
            ref = rcv.at[k, dx]
            pltpu.make_async_remote_copy(
                ref, ref, send_sem.at[0], rcv_sem.at[k * 4 + dx], device_id=twin, device_id_type=MESH
            ).wait_recv()
        chunk = ((x - dx + 4) % 4) * 2
        own = cst[0, dx * 2 + kept, mine] + rcv[0, dx].astype(jnp.float32)
        other = rcv[1, dx].astype(jnp.float32) + rcv[2, dx].astype(jnp.float32)
        lanes = pl.ds(pl.multiple_of((chunk + yl) * LANES, LANES), LANES)
        out_ref[:, lanes] = own.astype(jnp.bfloat16)
        turned[lanes, :] = own.T.astype(jnp.bfloat16)
        lanes = pl.ds(pl.multiple_of((chunk + 1 - yl) * LANES, LANES), LANES)
        out_ref[:, lanes] = other.astype(jnp.bfloat16)
        turned[lanes, :] = other.T.astype(jnp.bfloat16)

    def relay_tests(a):
        for h in range(2):
            tests_arrived(h, a, 1)
            tests_arrived(h, a, 3)
            test_hop(h, 1, a, 1, 1, part=0)
            test_hop(h, 1, a, 3, -1, part=1)

    def gradients(t):
        landed(gbuf.at[1, pl.ds(t * TILE, TILE)], g_sem.at[t])

    each(1, 0)
    each(3, 0)
    for h in range(2):
        hop(h, 0, 1, 0, 1, part=0)
        hop(h, 0, 3, 0, -1, part=1)
    for a in (1, 3):
        for h in range(2):
            for way in (1, -1):
                hop(h, 1, a, 0, way)
    each(0, 1)
    each(0, 3)
    for h in range(2):
        hop(h, 1, 0, 1, 1, part=0)
        hop(h, 1, 0, 3, -1, part=1)
    tests_arrived(1, 0, 0)
    for axis in range(2):
        for h in range(2):
            for way in (1, -1):
                test_hop(h, axis, 0, 0, way)
    multiply(0, 0, 0)
    each(2, 0)
    for h in range(2):
        for way in (1, -1):
            hop(h, 1, 2, 0, way)
    add_twin(0, 0, 0)
    for a in (1, 3):
        each(a, 1)
        each(a, 3)
        for h in range(2):
            hop(h, 1, a, 1, 1, part=0)
            hop(h, 1, a, 3, -1, part=1)
        if a == 1:
            multiply(0, 1, 0)
            gradients(0)
            tile(1, 0, 0, 0)
            tile(1, 1, 0, 0)
    for a in (1, 3):
        for h in range(2):
            tests_arrived(h, a, 0)
            tests_arrived(h, 0, a)
            way = 1 if a == 1 else -1
            test_hop(h, 0, a, 0, way, part=a // 2)
            test_hop(h, 1, 0, a, way, part=a // 2)
    add_twin(0, 1, 0)
    multiply(0, 3, 0)
    tile(1, 3, 0, 0)
    each(0, 2)
    multiply(0, 0, 1)
    tile(1, 0, 1, 0)
    add_twin(0, 3, 0)
    each(2, 1)
    each(2, 3)
    for h in range(2):
        hop(h, 1, 2, 1, 1, part=0)
        hop(h, 1, 2, 3, -1, part=1)
    for a in (1, 3):
        for h in range(2):
            for way in (1, -1):
                test_hop(h, 1, a, 0, way)
    add_twin(0, 0, 1)
    each(1, 2)
    multiply(0, 1, 1)
    multiply(0, 2, 0)
    tile(1, 1, 1, 0)
    tile(1, 2, 0, 0)
    add_twin(0, 1, 1)
    add_twin(0, 2, 0)
    for h in range(2):
        tests_arrived(h, 2, 0)
        for way in (1, -1):
            test_hop(h, 1, 2, 0, way)
    gradients(1)
    before = None
    for now in ((0, 0), (0, 1), (1, 0), (1, 1), (3, 0), (2, 0)):
        tile(1, *now, 1)
        to_other_core(1, *now)
        if before is not None:
            add_twin(1, *before)
        before = now
    each(3, 2)
    multiply(0, 3, 1)
    add_twin(1, *before)
    multiply(1, 3, 1)
    add_twin(0, 3, 1)
    add_twin(1, 3, 1)
    each(2, 2)
    multiply(0, 2, 1)
    relay_tests(1)
    multiply(1, 2, 1)
    relay_tests(3)
    add_twin(0, 2, 1)
    add_twin(1, 2, 1)
    relay_tests(2)
    finish(0)
    finish(1)
    finish(3)
    for h in range(2):
        for a in range(4):
            tests_arrived(h, a, 2)
    finish(2)

    def score(quarter, i):
        rows = pl.ds(pl.multiple_of(quarter * 256 + i * LANES, LANES), LANES)
        part_scores[quarter, pl.ds(i * LANES, LANES), :] = jnp.dot(
            tall[rows, :], turned[...], preferred_element_type=jnp.float32
        )

    def to_twin(quarter, k, i):
        rows = pl.ds(i * LANES, LANES)
        send(
            part_scores.at[quarter, rows], twin_scores.at[k, rows], score_sem.at[k * 2 + i], twin
        )

    def twin_sum(quarter, k, i):
        rows = pl.ds(i * LANES, LANES)
        landed(twin_scores.at[k, rows], score_sem.at[k * 2 + i])
        return part_scores[quarter, rows, :] + twin_scores[k, rows, :]

    far, near = (1 - yh) * 2, yh * 2
    for i in range(2):
        score(far + 1 - c, i)
        to_twin(far + 1 - c, 0, i)
    for i in range(2):
        score(far + c, i)
        total = twin_sum(far + c, 0, i).astype(jnp.bfloat16)
        for k in range(2):
            away_scores[i, k] = total[k * 64 : k * 64 + 64]
        for k in range(2):
            send(
                away_scores.at[i, k], relay_scores.at[i, k],
                score_sem.at[4 + i * 2 + k], ways[i],
            )
    for i in range(2):
        score(near + 1 - c, i)
        to_twin(near + 1 - c, 1, i)
    for i in range(2):
        score(near + c, i)
    for k in range(2):
        for i in range(2):
            landed(relay_scores.at[i, k], score_sem.at[4 + i * 2 + k])
            send(
                relay_scores.at[i, k], far_scores.at[i, k], score_sem.at[8 + i * 2 + k],
                ways[1 - i],
            )
    for i in range(2):
        score_ref[pl.ds(i * LANES, LANES), :] = twin_sum(near + c, 1, i)
    for k in range(2):
        for i in range(2):
            landed(far_scores.at[i, k], score_sem.at[8 + i * 2 + k])
            rows = pl.ds(i * LANES + k * 64, 64)
            score_ref[rows, :] = score_ref[rows, :] + far_scores[i, k].astype(jnp.float32)
    for copy in sent:
        if copy is not None:
            copy.wait_send()
    for copy, keep in given:
        @pl.when(jnp.logical_not(keep))
        def _():
            copy.wait_send()


def local(train_grads, projection, test_features, example_weights):
    flops = 2 * 2 * ROWS * DEPTH * 2048
    inner, projected = pl.pallas_call(
        project_kernel,
        out_shape=(
            jax.ShapeDtypeStruct((256, ROWS), jnp.float32),
            jax.ShapeDtypeStruct((ROWS, 1024), jnp.bfloat16),
        ),
        in_specs=[pl.BlockSpec(memory_space=pltpu.HBM)] * 3,
        out_specs=(pl.BlockSpec(memory_space=pltpu.VMEM),) * 2,
        scratch_shapes=[
            pltpu.VMEM((2, 4, 4, HALF, LANES), jnp.bfloat16),
            pltpu.VMEM((2, ROWS, DEPTH), jnp.bfloat16),
            pltpu.VMEM((2, 8, 2, ROWS, LANES), jnp.float32),
            pltpu.VMEM((2, 8, ROWS, LANES), jnp.float32),
            pltpu.VMEM((2, 8, ROWS, LANES), jnp.bfloat16),
            pltpu.VMEM((3, 4, ROWS, LANES), jnp.bfloat16),
            pltpu.VMEM((1024, 1024), jnp.bfloat16),
            pltpu.VMEM((1024, ROWS), jnp.bfloat16),
            pltpu.VMEM((4, 256, ROWS), jnp.float32),
            pltpu.VMEM((2, 256, ROWS), jnp.float32),
            pltpu.VMEM((2, 2, 64, ROWS), jnp.bfloat16),
            pltpu.VMEM((2, 2, 64, ROWS), jnp.bfloat16),
            pltpu.VMEM((2, 2, 64, ROWS), jnp.bfloat16),
            pltpu.SemaphoreType.DMA((4,)),
            pltpu.SemaphoreType.DMA((160,)),
            pltpu.SemaphoreType.DMA((32,)),
            pltpu.SemaphoreType.DMA((TILES,)),
            pltpu.SemaphoreType.DMA((16,)),
            pltpu.SemaphoreType.DMA((12,)),
            pltpu.SemaphoreType.DMA((32,)),
            pltpu.SemaphoreType.DMA((12,)),
        ],
        compiler_params=pltpu.CompilerParams(
            collective_id=0, has_side_effects=True, vmem_limit_bytes=44 * 1024 * 1024
        ),
        cost_estimate=pl.CostEstimate(
            flops=flops, bytes_accessed=8 * 2**20, transcendentals=0
        ),
    )(*[pltpu.with_memory_space_constraint(v, pltpu.HBM) for v in (train_grads, projection, test_features)])
    return inner * example_weights[None, :], projected


def solution(mesh):
    return jax.shard_map(
        local,
        mesh=mesh,
        in_specs=(P("ex", "feat"), P("feat", "ex"), P("ex", "feat"), P("ex")),
        out_specs=(P("feat", "ex"), P("ex", "feat")),
        check_vma=False,
    )
```
